64 devices in a mesh: dp: 4 (over x, y), cp: 16 (over z, core).
Axes of the slice: x: 2, y: 2, z: 8, core: 2. Of those that a mesh axis runs over, the one named last changes fastest.
The devices are a block of a 4x4x8 slice.
Arguments:
- q_tok: bfloat16 [32768, 8, 128], P(('dp', 'cp')), parts along dimension 0
- k_tok: bfloat16 [32768, 128], P(('dp', 'cp')), parts along dimension 0
- v_tok: bfloat16 [32768, 128], P(('dp', 'cp')), parts along dimension 0
- fwd_out: bfloat16 [32768, 8, 128], P(('dp', 'cp')), parts along dimension 0
- d_out: bfloat16 [32768, 8, 128], P(('dp', 'cp')), parts along dimension 0
- lse_row: float32 [32768, 8], P(('dp', 'cp')), parts along dimension 0
Outputs:
- output 1: bfloat16 [32768, 8, 128], P(('dp', 'cp')), parts along dimension 0
- output 2: bfloat16 [32768, 128], P(('dp', 'cp')), parts along dimension 0
- output 3: bfloat16 [32768, 128], P(('dp', 'cp')), parts along dimension 0
There are 4 independent parts. The reference program is written for one: setup_inputs(seed, part) draws one part's arguments, and reference() takes and returns one part's arrays. A program takes and returns all parts, laid end to end along the dimension named above; each array names one.
All inputs are finite; a program needn't handle non-finite values.
Results may differ from the reference program's by a relative error of at most 0.001.
Values are sent between devices in bfloat16 or wider.
A program may use at most 768 MiB of HBM per device.

```python
import jax
import jax.numpy as jnp
from jax import lax

TOK_DEV = 512
CP = 16
GQA = 8
HEAD = 128

SEQ = CP * TOK_DEV
Q_BLOCK = min(TOK_DEV, 128)
SOFTMAX_SCALE = HEAD ** -0.5
GRAD_GAIN = 0.25 * SEQ ** 0.5


def attention_forward(q_tok, k_tok, v_tok):
    k_full = k_tok.astype(jnp.float32)
    v_full = v_tok.astype(jnp.float32)
    columns = jnp.arange(SEQ)
    n_blocks = SEQ // Q_BLOCK

    def one_block(block_in):
        q_block, row_ids = block_in
        logits = jnp.einsum('rgd,cd->rgc', q_block.astype(jnp.float32), k_full) * SOFTMAX_SCALE
        allowed = columns[None, :] <= row_ids[:, None]
        logits = jnp.where(allowed[:, None, :], logits, -jnp.inf)
        lse_block = jax.nn.logsumexp(logits, axis=-1)
        prob_mat = jnp.exp(logits - lse_block[:, :, None])
        out_block = jnp.einsum('rgc,cd->rgd', prob_mat, v_full)
        return out_block.astype(jnp.bfloat16), lse_block

    out_blocks, lse_blocks = lax.map(one_block, (q_tok.reshape(n_blocks, Q_BLOCK, GQA, HEAD), columns.reshape(n_blocks, Q_BLOCK)))
    return out_blocks.reshape(SEQ, GQA, HEAD), lse_blocks.reshape(SEQ, GQA)


def setup_inputs(seed: int = 0, part: int = 0) -> dict:
    base_key = jax.random.fold_in(jax.random.key(seed), part)
    key_q, key_k, key_v, key_m, key_g = jax.random.split(base_key, 5)
    q_tok = jax.random.normal(key_q, (SEQ, GQA, HEAD), jnp.float32).astype(jnp.bfloat16)
    k_tok = jax.random.normal(key_k, (SEQ, HEAD), jnp.float32).astype(jnp.bfloat16)
    v_mean = jax.random.normal(key_m, (HEAD,), jnp.float32)
    v_tok = (v_mean[None, :] + jax.random.normal(key_v, (SEQ, HEAD), jnp.float32)).astype(jnp.bfloat16)
    d_out = (GRAD_GAIN * jax.random.normal(key_g, (SEQ, GQA, HEAD), jnp.float32)).astype(jnp.bfloat16)
    fwd_out, lse_row = attention_forward(q_tok, k_tok, v_tok)
    return {'q_tok': q_tok, 'k_tok': k_tok, 'v_tok': v_tok, 'fwd_out': fwd_out, 'd_out': d_out, 'lse_row': lse_row}


def reference(q_tok, k_tok, v_tok, fwd_out, d_out, lse_row):
    row_delta = jnp.sum(d_out.astype(jnp.float32) * fwd_out.astype(jnp.float32), axis=-1)
    k_full = k_tok.astype(jnp.float32)
    v_full = v_tok.astype(jnp.float32)
    columns = jnp.arange(SEQ)
    n_blocks = SEQ // Q_BLOCK

    def one_block(carry, block_in):
        dk_acc, dv_acc = carry
        q_block, do_block, lse_block, delta_block, row_ids = block_in
        q_wide = q_block.astype(jnp.float32)
        do_wide = do_block.astype(jnp.float32)
        logits = jnp.einsum('rgd,cd->rgc', q_wide, k_full) * SOFTMAX_SCALE
        allowed = columns[None, :] <= row_ids[:, None]
        prob_mat = jnp.exp(jnp.where(allowed[:, None, :], logits - lse_block[:, :, None], -jnp.inf))
        d_prob = jnp.einsum('rgd,cd->rgc', do_wide, v_full)
        d_score = prob_mat * (d_prob - delta_block[:, :, None])
        prob_low = prob_mat.astype(jnp.bfloat16).astype(jnp.float32)
        score_low = d_score.astype(jnp.bfloat16).astype(jnp.float32)
        dq_block = jnp.einsum('rgc,cd->rgd', score_low, k_full) * SOFTMAX_SCALE
        dk_acc = dk_acc + jnp.einsum('rgc,rgd->cd', score_low, q_wide)
        dv_acc = dv_acc + jnp.einsum('rgc,rgd->cd', prob_low, do_wide)
        return (dk_acc, dv_acc), dq_block.astype(jnp.bfloat16)

    acc_start = (jnp.zeros((SEQ, HEAD), jnp.float32), jnp.zeros((SEQ, HEAD), jnp.float32))
    block_inputs = (q_tok.reshape(n_blocks, Q_BLOCK, GQA, HEAD), d_out.reshape(n_blocks, Q_BLOCK, GQA, HEAD), lse_row.reshape(n_blocks, Q_BLOCK, GQA), row_delta.reshape(n_blocks, Q_BLOCK, GQA), columns.reshape(n_blocks, Q_BLOCK))
    (dk_acc, dv_acc), dq_blocks = lax.scan(one_block, acc_start, block_inputs)
    grad_q = dq_blocks.reshape(SEQ, GQA, HEAD)
    grad_k = (dk_acc * SOFTMAX_SCALE).astype(jnp.bfloat16)
    grad_v = dv_acc.astype(jnp.bfloat16)
    return (grad_q, grad_k, grad_v)
```

```python
import functools

import jax
import jax.numpy as jnp
from jax import lax
from jax.experimental import pallas as pl
from jax.experimental.pallas import tpu as pltpu
from jax.sharding import PartitionSpec as P

MESH = pl.DeviceIdType.MESH
LOG2E = 1.4426950408889634
F32, BF16 = jnp.float32, jnp.bfloat16
CHUNK = 512
UNIT = 4
GROUP = CHUNK * UNIT
UP, DOWN = 4, 3
OFFSETS = (0, 1, -2, -4, 3, -3, 2, -1)


def dot_nt(a, b):
    return lax.dot_general(a, b, (((1,), (1,)), ((), ())), preferred_element_type=F32)


def dot_tn(a, b):
    return lax.dot_general(a, b, (((0,), (0,)), ((), ())), preferred_element_type=F32)


def dot_nn(a, b):
    return jnp.dot(a, b, preferred_element_type=F32)


def kernel(n, scale, q_hbm, k_hbm, v_hbm, do_hbm, lse_hbm, dl_hbm, dq_out, dk_out, dv_out,
           q_all, do_all, lse_all, dl_all, kv_all, part, dq_all, dq_in, up_buf, dn_buf,
           load_sem, xs_sem, xr_sem, agu_s, agu_r, agd_s, agd_r, rsd_s, rsd_r, rsu_s, rsu_r, dqs_sem, dqr_sem):
    chips = n // 2
    me = lax.axis_index('cp')
    z = me // 2
    core = me % 2
    rows = q_hbm.shape[0]
    groups = rows // GROUP
    cols = k_hbm.shape[0]
    wrap = lambda i: lax.rem(i + 2 * chips, chips)
    above = {'cp': 2 * wrap(z + 1) + core}
    below = {'cp': 2 * wrap(z - 1) + core}
    sibling = {'cp': 2 * z + 1 - core}

    def need(chip, y):
        return wrap(y) < wrap(chip)

    def any_of(flags):
        return functools.reduce(jnp.logical_or, flags)

    def up_on(d, z0):
        return any_of([need(z0 + i, z0 - d) for i in range(UP - d + 1)])

    def dn_on(e, z0):
        return any_of([need(z0 - i, z0 + e) for i in range(DOWN - e + 1)])

    def remote(src, dst, ss, rs, to):
        return pltpu.make_async_remote_copy(src_ref=src, dst_ref=dst, send_sem=ss, recv_sem=rs, device_id=to, device_id_type=MESH)

    def ag_up(d):
        blk = kv_all.at[wrap(z - d + 1)]
        return remote(blk, blk, agu_s.at[d - 1], agu_r.at[d - 1], above)

    def ag_up_in(d):
        blk = kv_all.at[wrap(z - d)]
        return remote(blk, blk, agu_s.at[d - 1], agu_r.at[d - 1], above)

    def ag_dn(e):
        blk = kv_all.at[wrap(z + e - 1)]
        return remote(blk, blk, agd_s.at[e - 1], agd_r.at[e - 1], below)

    def ag_dn_in(e):
        blk = kv_all.at[wrap(z + e)]
        return remote(blk, blk, agd_s.at[e - 1], agd_r.at[e - 1], below)

    def rs_dn(d):
        return remote(part.at[wrap(z - d)], dn_buf.at[d - 1], rsd_s.at[d - 1], rsd_r.at[d - 1], below)

    def rs_up(e):
        return remote(part.at[wrap(z + e)], up_buf.at[e - 1], rsu_s.at[e - 1], rsu_r.at[e - 1], above)

    srcs = (q_hbm, do_hbm, lse_hbm, dl_hbm)
    dsts = (q_all, do_all, lse_all, dl_all)

    def swap(i, g):
        r = pl.ds(g * GROUP, GROUP)
        return remote(srcs[i].at[r], dsts[i].at[pl.ds(rows + g * GROUP, GROUP)], xs_sem.at[i, g], xr_sem.at[i, g], sibling)

    def load(i):
        return pltpu.make_async_copy(srcs[i], dsts[i].at[pl.ds(0, rows)], load_sem.at[i])

    def dq_swap():
        return remote(dq_all.at[pl.ds(rows, rows)], dq_in, dqs_sem, dqr_sem, sibling)

    load_k = pltpu.make_async_copy(k_hbm, kv_all.at[z, 0], load_sem.at[4])
    load_v = pltpu.make_async_copy(v_hbm, kv_all.at[z, 1], load_sem.at[5])
    load_k.start()
    load_v.start()
    for i in range(4):
        load(i).start()

    barrier = pltpu.get_barrier_semaphore()
    for peer in (above, below, sibling):
        pl.semaphore_signal(barrier, inc=1, device_id=peer, device_id_type=MESH)
    pl.semaphore_wait(barrier, 3)

    load_k.wait()
    load_v.wait()
    pl.when(up_on(1, z + 1))(lambda: ag_up(1).start())
    pl.when(dn_on(1, z - 1))(lambda: ag_dn(1).start())
    for g in range(groups):
        for i in range(4):
            swap(i, g).start()

    part[...] = jnp.zeros_like(part)
    dq_all[...] = jnp.zeros_like(dq_all)
    for i in range(4):
        load(i).wait()

    def tiles(y, base, units, mask_from):
        k = kv_all[y, 0]
        v = kv_all[y, 1]
        ps, dss = [], []
        for u in range(units):
            r = pl.ds(pl.multiple_of(base + u * CHUNK, CHUNK), CHUNK)
            s = dot_nt(q_all[r, :], k)
            dp = dot_nt(do_all[r, :], v)
            p = jnp.exp2(s * (scale * LOG2E) - jnp.tile(lse_all[r, :], (1, cols // 128)))
            if mask_from is not None:
                row = lax.broadcasted_iota(jnp.int32, p.shape, 0) + u * CHUNK
                col = lax.broadcasted_iota(jnp.int32, p.shape, 1) * 8 - mask_from
                p = jnp.where(col <= row, p, 0.0)
            dss.append((p * (dp - jnp.tile(dl_all[r, :], (1, cols // 128)))).astype(BF16))
            ps.append(p.astype(BF16))
        r = pl.ds(pl.multiple_of(base, CHUNK), CHUNK * units)
        ds = jnp.concatenate(dss, 0)
        part[y, 1] += dot_tn(do_all[r, :], jnp.concatenate(ps, 0))
        part[y, 0] += dot_tn(q_all[r, :], ds)
        dq_all[r, :] += dot_nn(ds, k)

    def diag(i, carry):
        base = i * (2 * CHUNK)
        tiles(z, base, 2, base)
        return carry

    lax.fori_loop(0, rows // (2 * CHUNK), diag, 0)

    def ag_step(d):
        @pl.when(up_on(d, z))
        def _():
            ag_up_in(d).wait_recv()
        if d < UP:
            pl.when(up_on(d + 1, z + 1))(lambda: ag_up(d + 1).start())
        if d <= DOWN:
            @pl.when(dn_on(d, z))
            def _():
                ag_dn_in(d).wait_recv()
        if d < DOWN:
            pl.when(dn_on(d + 1, z - 1))(lambda: ag_dn(d + 1).start())

    def rs_dn_step(d):
        if d < UP:
            @pl.when(up_on(d + 1, z + 1))
            def _():
                rs_dn(d + 1).wait_recv()
                part[wrap(z - d)] += dn_buf[d]
        pl.when(up_on(d, z))(lambda: rs_dn(d).start())

    def rs_up_step(e):
        if e < DOWN:
            @pl.when(dn_on(e + 1, z - 1))
            def _():
                rs_up(e + 1).wait_recv()
                part[wrap(z + e)] += up_buf[e]
        pl.when(dn_on(e, z))(lambda: rs_up(e).start())

    def swap_wait(g):
        for i in range(4):
            swap(i, g).wait_recv()

    hooks = {
        0: [lambda: swap_wait(0)],
        1: [lambda: swap_wait(1), lambda: ag_step(1)],
        5: [lambda: ag_step(2)],
        8: [lambda: ag_step(3)],
        12: [lambda: ag_step(4)],
        16: [lambda: rs_dn_step(4)],
        20: [lambda: rs_up_step(3)],
        24: [lambda: rs_dn_step(3)],
        27: [lambda: rs_dn_step(2)],
        28: [lambda: rs_up_step(2)],
        30: [lambda: dq_swap().start()],
        31: [lambda: rs_up_step(1)],
    }

    def sweep(t, carry):
        w = t // 4
        j = t % 4
        for at, fns in hooks.items():
            @pl.when(t == at)
            def _():
                for fn in fns:
                    fn()
        off = sum(jnp.where(w == i, o, 0) for i, o in enumerate(OFFSETS))
        y = wrap(z + off)
        mine = j // 2
        on = jnp.logical_or(jnp.logical_and(w > 0, need(z, y)), jnp.logical_and(w == 0, jnp.logical_and(mine == 0, core == 0)))

        @pl.when(on)
        def _():
            tiles(y, (1 - mine) * rows + (j % 2) * GROUP, UNIT, None)
        return carry

    lax.fori_loop(0, 4 * len(OFFSETS), sweep, 0)
    rs_dn_step(1)

    dq_swap().wait_recv()
    for g in range(rows // CHUNK):
        r = pl.ds(g * CHUNK, CHUNK)
        dq_out[r, :] = ((dq_all[r, :] + dq_in[r, :]) * scale).astype(BF16)

    @pl.when(up_on(1, z + 1))
    def _():
        rs_dn(1).wait_recv()
        part[z] += dn_buf[0]

    @pl.when(dn_on(1, z - 1))
    def _():
        rs_up(1).wait_recv()
        part[z] += up_buf[0]

    dk_out[...] = (part[z, 0] * scale).T.astype(BF16)
    dv_out[...] = part[z, 1].T.astype(BF16)

    for g in range(groups):
        for i in range(4):
            swap(i, g).wait_send()
    for d in range(1, UP + 1):
        pl.when(up_on(d, z + 1))(lambda d=d: ag_up(d).wait_send())
        pl.when(up_on(d, z))(lambda d=d: rs_dn(d).wait_send())
    for e in range(1, DOWN + 1):
        pl.when(dn_on(e, z - 1))(lambda e=e: ag_dn(e).wait_send())
        pl.when(dn_on(e, z))(lambda e=e: rs_up(e).wait_send())
    dq_swap().wait_send()


def solution(mesh):
    n = mesh.shape['cp']
    row_spec = P(('dp', 'cp'))

    def local_fn(q_tok, k_tok, v_tok, fwd_out, d_out, lse_row):
        toks, heads, dim = q_tok.shape
        rows = toks * heads
        scale = dim ** -0.5
        delta = jnp.einsum('rgd,rgd->rg', d_out, fwd_out, preferred_element_type=F32)
        wide = lambda x: jnp.broadcast_to(x[:, :, None], (toks, heads, 128)).reshape(rows, 128)
        flat = lambda x: x.reshape(rows, dim)
        chips = n // 2
        groups = rows // GROUP
        dma = pltpu.SemaphoreType.DMA
        dq, dk, dv = pl.pallas_call(
            functools.partial(kernel, n, scale),
            out_shape=(jax.ShapeDtypeStruct((rows, dim), BF16), jax.ShapeDtypeStruct((toks, dim), BF16), jax.ShapeDtypeStruct((toks, dim), BF16)),
            in_specs=[pl.BlockSpec(memory_space=pl.ANY)] * 6,
            out_specs=[pl.BlockSpec(memory_space=pltpu.VMEM)] * 3,
            scratch_shapes=[
                pltpu.VMEM((2 * rows, dim), BF16),
                pltpu.VMEM((2 * rows, dim), BF16),
                pltpu.VMEM((2 * rows, 128), F32),
                pltpu.VMEM((2 * rows, 128), F32),
                pltpu.VMEM((chips, 2, toks, dim), BF16),
                pltpu.VMEM((chips, 2, dim, toks), F32),
                pltpu.VMEM((2 * rows, dim), F32),
                pltpu.VMEM((rows, dim), F32),
                pltpu.VMEM((DOWN, 2, dim, toks), F32),
                pltpu.VMEM((UP, 2, dim, toks), F32),
                dma((6,)), dma((4, groups)), dma((4, groups)),
                dma((UP,)), dma((UP,)), dma((DOWN,)), dma((DOWN,)),
                dma((UP,)), dma((UP,)), dma((DOWN,)), dma((DOWN,)),
                dma, dma,
            ],
            compiler_params=pltpu.CompilerParams(collective_id=0, has_side_effects=True, vmem_limit_bytes=60 * 2 ** 20),
        )(flat(q_tok), k_tok, v_tok, flat(d_out), wide(lse_row * LOG2E), wide(delta))
        return dq.reshape(q_tok.shape), dk, dv

    return jax.shard_map(local_fn, mesh=mesh, in_specs=(row_spec,) * 6, out_specs=(row_spec,) * 3, check_vma=False)
```

```python
import functools

import jax
import jax.numpy as jnp
from jax import lax
from jax.experimental import pallas as pl
from jax.experimental.pallas import tpu as pltpu
from jax.sharding import PartitionSpec as P

MESH = pl.DeviceIdType.MESH
LOG2E = 1.4426950408889634
F32, BF16 = jnp.float32, jnp.bfloat16
CHUNK = 512
UNIT = 4
GROUP = CHUNK * UNIT
UP, DOWN = (4, 3), (3, 4)
FAR = 4
OFFSETS = (1, -2, -4, -3, 3, 2, -1)


def dot_nt(a, b):
    return lax.dot_general(a, b, (((1,), (1,)), ((), ())), preferred_element_type=F32)


def dot_tn(a, b):
    return lax.dot_general(a, b, (((0,), (0,)), ((), ())), preferred_element_type=F32)


def dot_nn(a, b):
    return jnp.dot(a, b, preferred_element_type=F32)


def kernel(n, scale, q_hbm, k_hbm, v_hbm, out_hbm, do_hbm, lse_in, dq_out, dk_out, dv_out,
           q_all, do_all, fwd, lse_all, dl_all, stats, kv_all, part, dq_all, dq_in, up_buf, dn_buf,
           load_sem, xs_sem, xr_sem, agu_s, agu_r, agd_s, agd_r, rsd_s, rsd_r, rsu_s, rsu_r, dqs_sem, dqr_sem):
    chips = n // 2
    me = lax.axis_index('cp')
    z = me // 2
    core = me % 2
    rows = q_hbm.shape[0]
    halves = rows // GROUP
    cols, dim = k_hbm.shape
    heads = rows // cols
    wrap = lambda i: lax.rem(i + 2 * chips, chips)
    above = {'cp': 2 * wrap(z + 1) + core}
    below = {'cp': 2 * wrap(z - 1) + core}
    sibling = {'cp': 2 * z + 1 - core}

    def need(chip, y):
        return wrap(y) < wrap(chip)

    def any_of(flags):
        return functools.reduce(jnp.logical_or, flags)

    def up_on(d, z0, p):
        return any_of([need(z0 + i, z0 - d) for i in range(UP[p] - d + 1)])

    def dn_on(e, z0, p):
        return any_of([need(z0 - i, z0 + e) for i in range(DOWN[p] - e + 1)])

    def remote(src, dst, ss, rs, to):
        return pltpu.make_async_remote_copy(src_ref=src, dst_ref=dst, send_sem=ss, recv_sem=rs, device_id=to, device_id_type=MESH)

    def ag_up(d, p, dist):
        blk = kv_all.at[wrap(z - dist), p]
        return remote(blk, blk, agu_s.at[d - 1, p], agu_r.at[d - 1, p], above)

    def ag_dn(e, p, dist):
        blk = kv_all.at[wrap(z + dist), p]
        return remote(blk, blk, agd_s.at[e - 1, p], agd_r.at[e - 1, p], below)

    def rs_dn(d, p):
        return remote(part.at[wrap(z - d), p], dn_buf.at[d - 1, p], rsd_s.at[d - 1, p], rsd_r.at[d - 1, p], below)

    def rs_up(e, p):
        return remote(part.at[wrap(z + e), p], up_buf.at[e - 1, p], rsu_s.at[e - 1, p], rsu_r.at[e - 1, p], above)

    def swap(i, g):
        src, dst = ((q_hbm, q_all), (do_hbm, do_all))[i]
        return remote(src.at[pl.ds(g * GROUP, GROUP)], dst.at[pl.ds(rows + g * GROUP, GROUP)], xs_sem.at[i, g], xr_sem.at[i, g], sibling)

    def swap_stats():
        return remote(stats.at[0], stats.at[1], xs_sem.at[2, 0], xr_sem.at[2, 0], sibling)

    def dq_swap():
        return remote(dq_all.at[pl.ds(rows, rows)], dq_in, dqs_sem, dqr_sem, sibling)

    local = [
        pltpu.make_async_copy(k_hbm, kv_all.at[z, 0], load_sem.at[0]),
        pltpu.make_async_copy(v_hbm, kv_all.at[z, 1], load_sem.at[1]),
        pltpu.make_async_copy(do_hbm, do_all.at[pl.ds(0, rows)], load_sem.at[2]),
        pltpu.make_async_copy(out_hbm, fwd, load_sem.at[3]),
        pltpu.make_async_copy(q_hbm, q_all.at[pl.ds(0, rows)], load_sem.at[4]),
    ]
    for c in local:
        c.start()

    barrier = pltpu.get_barrier_semaphore()
    for peer in (above, below, sibling):
        pl.semaphore_signal(barrier, inc=1, device_id=peer, device_id_type=MESH)
    pl.semaphore_wait(barrier, 3)

    for p in range(2):
        local[p].wait()
        pl.when(up_on(1, z + 1, p))(lambda: ag_up(1, p, 0).start())
        pl.when(dn_on(1, z - 1, p))(lambda: ag_dn(1, p, 0).start())
    for g in range(halves):
        for i in range(2):
            swap(i, g).start()

    def widen(x, dst, base):
        for t in range(128):
            dst[pl.ds(pl.multiple_of(base + t * heads, heads), heads), :] = jnp.broadcast_to(x[:, t:t + 1], (heads, 128))

    local[2].wait()
    local[3].wait()
    stats[0, 0] = lse_in[...] * LOG2E
    lane = lax.broadcasted_iota(jnp.int32, (heads, 128), 1)

    def own_stats(i, carry):
        at = pl.ds(pl.multiple_of(i * 128, 128), 128)
        base = i * (128 * heads)
        r = pl.ds(pl.multiple_of(base, 128 * heads), 128 * heads)
        d = jnp.sum(do_all[r, :].astype(F32) * fwd[r, :].astype(F32), axis=-1, keepdims=True)
        wide = jnp.broadcast_to(d, (128 * heads, 128))
        dl_all[r, :] = wide
        dense = jnp.zeros((heads, 128), F32)
        for t in range(128):
            dense = jnp.where(lane == t, wide[t * heads:(t + 1) * heads], dense)
        stats[0, 1, :, at] = dense
        widen(stats[0, 0, :, at], lse_all, base)
        return carry

    lax.fori_loop(0, cols // 128, own_stats, 0)
    local[4].wait()
    part[...] = jnp.zeros_like(part)
    dq_all[...] = jnp.zeros_like(dq_all)
    swap_stats().start()

    def tiles(y, base, units, width, mask_from):
        k = kv_all[y, 0, :width]
        v = kv_all[y, 1, :width]
        ps, dss = [], []
        for u in range(units):
            r = pl.ds(pl.multiple_of(base + u * CHUNK, CHUNK), CHUNK)
            s = dot_nt(q_all[r, :], k)
            dp = dot_nt(do_all[r, :], v)
            p = jnp.exp2(s * (scale * LOG2E) - jnp.tile(lse_all[r, :], (1, width // 128)))
            if mask_from is not None:
                row = lax.broadcasted_iota(jnp.int32, p.shape, 0) + u * CHUNK
                col = lax.broadcasted_iota(jnp.int32, p.shape, 1) * heads - mask_from
                p = jnp.where(col <= row, p, 0.0)
            dss.append((p * (dp - jnp.tile(dl_all[r, :], (1, width // 128)))).astype(BF16))
            ps.append(p.astype(BF16))
        r = pl.ds(pl.multiple_of(base, CHUNK), CHUNK * units)
        ds = jnp.concatenate(dss, 0)
        part[y, 1, :, :width] += dot_tn(do_all[r, :], jnp.concatenate(ps, 0))
        part[y, 0, :, :width] += dot_tn(q_all[r, :], ds)
        dq_all[r, :] += dot_nn(ds, k)

    pairs = rows // (2 * CHUNK)

    def diag(width, i, carry):
        base = i * (2 * CHUNK)
        tiles(z, base, 2, width, base)
        return carry

    lax.fori_loop(0, pairs // 2, functools.partial(diag, cols // 2), 0)
    lax.fori_loop(pairs // 2, pairs, functools.partial(diag, cols), 0)

    swap_stats().wait_recv()

    def sibling_stats(i, carry):
        at = pl.ds(pl.multiple_of(i * 128, 128), 128)
        base = rows + i * (128 * heads)
        widen(stats[1, 0, :, at], lse_all, base)
        widen(stats[1, 1, :, at], dl_all, base)
        return carry

    lax.fori_loop(0, cols // 128, sibling_stats, 0)

    def ag_step(d):
        for p in range(2):
            if d <= UP[p]:
                pl.when(up_on(d, z, p))(lambda: ag_up(d, p, d).wait_recv())
            if d < UP[p]:
                pl.when(up_on(d + 1, z + 1, p))(lambda: ag_up(d + 1, p, d).start())
            if d <= DOWN[p]:
                pl.when(dn_on(d, z, p))(lambda: ag_dn(d, p, d).wait_recv())
            if d < DOWN[p]:
                pl.when(dn_on(d + 1, z - 1, p))(lambda: ag_dn(d + 1, p, d).start())

    def step(d, p, reach, is_on, step_out, buf, y, away, early):
        comes = is_on(d + 1, z + away, p) if d < reach else None
        if early:
            go = is_on(d, z, p)
            if comes is not None:
                go = jnp.logical_and(go, jnp.logical_not(comes))
            pl.when(go)(lambda: step_out(d, p).start())
        elif comes is not None:
            @pl.when(comes)
            def _():
                step_out(d + 1, p).wait_recv()
                part[y, p] += buf[d, p]
                step_out(d, p).start()

    def dn(d, p, early):
        step(d, p, UP[p], up_on, rs_dn, dn_buf, wrap(z - d), 1, early)

    def up(e, p, early):
        step(e, p, DOWN[p], dn_on, rs_up, up_buf, wrap(z + e), -1, early)

    def both(f, d, p):
        f(d, p, True)
        f(d, p, False)

    def swap_wait():
        for g in range(halves):
            for i in range(2):
                swap(i, g).wait_recv()

    hooks = {
        0: lambda: (swap_wait(), ag_step(1)),
        3: lambda: ag_step(2),
        4: lambda: (up(1, 0, True), up(1, 1, True)),
        6: lambda: ag_step(3),
        8: lambda: (ag_step(4), dn(2, 0, True), dn(2, 1, True)),
        12: lambda: (both(dn, 4, 0), both(up, 4, 1)),
        16: lambda: (both(dn, 3, 0), both(dn, 3, 1)),
        19: lambda: dn(2, 0, False),
        20: lambda: (both(up, 3, 1), both(up, 3, 0)),
        21: lambda: dn(2, 1, False),
        24: lambda: (both(up, 2, 1), up(2, 0, True)),
        26: lambda: up(2, 0, False),
        27: lambda: up(1, 1, False),
        28: lambda: (both(dn, 1, 0), both(dn, 1, 1)),
    }

    def sweep(t, carry):
        w = t // 4
        j = t % 4
        for at, fn in hooks.items():
            @pl.when(t == at)
            def _():
                fn()
        off = sum(jnp.where(w == i, o, 0) for i, o in enumerate(OFFSETS))
        y = wrap(z + off)
        last = w == len(OFFSETS)
        on = jnp.logical_or(jnp.logical_and(jnp.logical_not(last), need(z, y)), jnp.logical_and(last, core == 0))

        @pl.when(on)
        def _():
            tiles(y, (1 - j // 2) * rows + (j % 2) * GROUP, UNIT, cols, None)
        return carry

    lax.fori_loop(0, 4 * len(OFFSETS) + 2, sweep, 0)
    dq_swap().start()
    up(1, 0, False)

    dq_swap().wait_recv()
    for g in range(rows // CHUNK):
        r = pl.ds(g * CHUNK, CHUNK)
        dq_out[r, :] = ((dq_all[r, :] + dq_in[r, :]) * scale).astype(BF16)

    for p in range(2):
        @pl.when(up_on(1, z + 1, p))
        def _():
            rs_dn(1, p).wait_recv()
            part[z, p] += dn_buf[0, p]

        @pl.when(dn_on(1, z - 1, p))
        def _():
            rs_up(1, p).wait_recv()
            part[z, p] += up_buf[0, p]

    dk_out[...] = (part[z, 0] * scale).T.astype(BF16)
    dv_out[...] = part[z, 1].T.astype(BF16)

    for g in range(halves):
        for i in range(2):
            swap(i, g).wait_send()
    swap_stats().wait_send()
    for p in range(2):
        for d in range(1, UP[p] + 1):
            pl.when(up_on(d, z + 1, p))(lambda: ag_up(d, p, d - 1).wait_send())
            pl.when(up_on(d, z, p))(lambda: rs_dn(d, p).wait_send())
        for e in range(1, DOWN[p] + 1):
            pl.when(dn_on(e, z - 1, p))(lambda: ag_dn(e, p, e - 1).wait_send())
            pl.when(dn_on(e, z, p))(lambda: rs_up(e, p).wait_send())
    dq_swap().wait_send()


def deliver(dq, dk, dv, dq_out, dk_out, dv_out, a, b, c, sem_in, sem_out):
    pieces = 4
    step = dq.shape[0] // pieces
    moves = [(dk, b, dk_out), (dv, c, dv_out)] + [tuple(x.at[pl.ds(i * step, step)] for x in (dq, a, dq_out)) for i in range(pieces)]
    ins = [pltpu.make_async_copy(s, m, sem_in.at[i]) for i, (s, m, _) in enumerate(moves)]
    outs = [pltpu.make_async_copy(m, d, sem_out.at[i]) for i, (_, m, d) in enumerate(moves)]
    for x in ins:
        x.start()
    for x, o in zip(ins, outs):
        x.wait()
        o.start()
    for o in outs:
        o.wait()


def solution(mesh):
    n = mesh.shape['cp']
    row_spec = P(('dp', 'cp'))

    def local_fn(q_tok, k_tok, v_tok, fwd_out, d_out, lse_row):
        toks, heads, dim = q_tok.shape
        rows = toks * heads
        scale = dim ** -0.5
        flat = lambda x: x.reshape(rows, dim)
        chips = n // 2
        halves = rows // GROUP
        dma = pltpu.SemaphoreType.DMA
        hbm, vmem = pl.BlockSpec(memory_space=pl.ANY), pl.BlockSpec(memory_space=pltpu.VMEM)
        shapes = (jax.ShapeDtypeStruct((rows, dim), BF16), jax.ShapeDtypeStruct((toks, dim), BF16), jax.ShapeDtypeStruct((toks, dim), BF16))
        hops = dma((FAR, 2))
        grads = pl.pallas_call(
            functools.partial(kernel, n, scale),
            out_shape=shapes,
            in_specs=[hbm] * 5 + [vmem],
            out_specs=[vmem] * 3,
            scratch_shapes=[
                pltpu.VMEM((2 * rows, dim), BF16),
                pltpu.VMEM((2 * rows, dim), BF16),
                pltpu.VMEM((rows, dim), BF16),
                pltpu.VMEM((2 * rows, 128), F32),
                pltpu.VMEM((2 * rows, 128), F32),
                pltpu.VMEM((2, 2, heads, toks), F32),
                pltpu.VMEM((chips, 2, toks, dim), BF16),
                pltpu.VMEM((chips, 2, dim, toks), F32),
                pltpu.VMEM((2 * rows, dim), F32),
                pltpu.VMEM((rows, dim), F32),
                pltpu.VMEM((FAR, 2, dim, toks), F32),
                pltpu.VMEM((FAR, 2, dim, toks), F32),
                dma((5,)), dma((3, halves)), dma((3, halves)),
                hops, hops, hops, hops, hops, hops, hops, hops,
                dma, dma,
            ],
            compiler_params=pltpu.CompilerParams(collective_id=0, has_side_effects=True, vmem_limit_bytes=60 * 2 ** 20),
        )(flat(q_tok), k_tok, v_tok, flat(fwd_out), flat(d_out), lse_row.T)
        dq, dk, dv = pl.pallas_call(
            deliver,
            out_shape=shapes,
            in_specs=[hbm] * 3,
            out_specs=[hbm] * 3,
            scratch_shapes=[pltpu.VMEM(s.shape, s.dtype) for s in shapes] + [dma((6,)), dma((6,))],
        )(*grads)
        return dq.reshape(q_tok.shape), dk, dv

    return jax.shard_map(local_fn, mesh=mesh, in_specs=(row_spec,) * 6, out_specs=(row_spec,) * 3, check_vma=False)
```

```python
import functools

import jax
import jax.numpy as jnp
from jax import lax
from jax.experimental import pallas as pl
from jax.experimental.pallas import tpu as pltpu
from jax.sharding import PartitionSpec as P

MESH = pl.DeviceIdType.MESH
LOG2E = 1.4426950408889634
F32, BF16 = jnp.float32, jnp.bfloat16
CHUNK = 512
UNIT = 4
GROUP = CHUNK * UNIT
UP, DOWN = (4, 3), (3, 4)
FAR = 4
OFFSETS = (-2, -3, -4, 3, 2, 1, -1)
SCHEDULE = {
    -2: (('ag', 1, 0),),
    -1: (('ag', 1, 1),),
    0: (('ag', 2, 0), ('ag', 2, 1),),
    4: (('ag', 3, 0), ('ag', 3, 1),),
    7: (('ag', 4, 0),),
    8: (('ag', 4, 1), ('dn', 3, 0, True), ('dn', 3, 1, True),),
    12: (('dn', 4, 0, True), ('up', 4, 1, True),),
    14: (('dn', 2, 0, True), ('dn', 2, 1, False),),
    16: (('up', 3, 1, False), ('dn', 3, 0, False), ('up', 3, 0, True), ('dn', 2, 0, False),),
    19: (('dn', 2, 1, True),),
    21: (('up', 2, 1, False),),
    23: (('up', 2, 0, False),),
    27: (('up', 1, 1, False),),
    28: (('dn', 1, 0, False),),
    29: (('up', 3, 1, True), ('up', 1, 0, True),),
    30: (('up', 1, 0, False), ('up', 1, 1, True),),
    32: (('dn', 1, 0, True), ('dn', 1, 1, False), ('dn', 1, 1, True),),
    34: (('up', 2, 0, True), ('up', 2, 1, True),),
}


def dot_nt(a, b):
    return lax.dot_general(a, b, (((1,), (1,)), ((), ())), preferred_element_type=F32)


def dot_tn(a, b):
    return lax.dot_general(a, b, (((0,), (0,)), ((), ())), preferred_element_type=F32)


def dot_nn(a, b):
    return jnp.dot(a, b, preferred_element_type=F32)


def kernel(n, scale, q_hbm, k_hbm, v_hbm, out_hbm, do_hbm, lse_in, dq_out, dk_out, dv_out,
           q_all, do_all, fwd, lse_all, dl_all, stats, kv_all, part, cross, dq_all, dq_in, up_buf, dn_buf,
           load_sem, xs_sem, xr_sem, agu_s, agu_r, agd_s, agd_r, rsd_s, rsd_r, rsu_s, rsu_r, dqs_sem, dqr_sem, cs_sem, cr_sem, home_s, home_r):
    chips = n // 2
    me = lax.axis_index('cp')
    z = me // 2
    core = me % 2
    rows = q_hbm.shape[0]
    halves = rows // GROUP
    cols, dim = k_hbm.shape
    heads = rows // cols
    wrap = lambda i: lax.rem(i + 2 * chips, chips)
    above = {'cp': 2 * wrap(z + 1) + core}
    below = {'cp': 2 * wrap(z - 1) + core}
    sibling = {'cp': 2 * z + 1 - core}

    def need(chip, y):
        return wrap(y) < wrap(chip)

    def any_of(flags):
        return functools.reduce(jnp.logical_or, flags)

    def up_on(d, z0, p):
        return any_of([need(z0 + i, z0 - d) for i in range(UP[p] - d + 1)])

    def dn_on(e, z0, p):
        return any_of([need(z0 - i, z0 + e) for i in range(DOWN[p] - e + 1)])

    def remote(src, dst, ss, rs, to):
        return pltpu.make_async_remote_copy(src_ref=src, dst_ref=dst, send_sem=ss, recv_sem=rs, device_id=to, device_id_type=MESH)

    def ag_up(d, p, dist):
        blk = kv_all.at[wrap(z - dist), p]
        return remote(blk, blk, agu_s.at[d - 1, p], agu_r.at[d - 1, p], above)

    def ag_dn(e, p, dist):
        blk = kv_all.at[wrap(z + dist), p]
        return remote(blk, blk, agd_s.at[e - 1, p], agd_r.at[e - 1, p], below)

    def rs_dn(d, p):
        return remote(part.at[wrap(z - d), p], dn_buf.at[d - 1, p], rsd_s.at[d - 1, p], rsd_r.at[d - 1, p], below)

    def rs_home(p, h):
        at = pl.ds(h * (cols // 2), cols // 2)
        return remote(part.at[wrap(z - 1), p, :, at], dn_buf.at[0, p, :, at], home_s.at[p, h], home_r.at[p, h], below)

    def home(h, early):
        comes = up_on(2, z + 1, 0)
        go = jnp.logical_and(up_on(1, z, 0), jnp.logical_not(comes)) if early else comes

        @pl.when(go)
        def _():
            for p in range(2):
                if not early and h == 0:
                    rs_dn(2, p).wait_recv()
                    part[wrap(z - 1), p] += dn_buf[1, p]
                rs_home(p, h).start()

    def rs_up(e, p):
        return remote(part.at[wrap(z + e), p], up_buf.at[e - 1, p], rsu_s.at[e - 1, p], rsu_r.at[e - 1, p], above)

    def swap(i, g):
        src, dst = ((q_hbm, q_all), (do_hbm, do_all))[i]
        return remote(src.at[pl.ds(g * GROUP, GROUP)], dst.at[pl.ds(rows + g * GROUP, GROUP)], xs_sem.at[i, g], xr_sem.at[i, g], sibling)

    def swap_stats():
        return remote(stats.at[0], stats.at[1], xs_sem.at[2, 0], xr_sem.at[2, 0], sibling)

    def cross_kv(p):
        return remote((k_hbm, v_hbm)[p], kv_all.at[chips, p], cs_sem.at[p], cr_sem.at[p], sibling)

    def cross_sum():
        return remote(part.at[chips], cross, cs_sem.at[2], cr_sem.at[2], sibling)

    def dq_swap():
        return remote(dq_all.at[pl.ds(rows, rows)], dq_in, dqs_sem, dqr_sem, sibling)

    def ag_step(d, p):
        if d <= UP[p]:
            pl.when(up_on(d, z, p))(lambda: ag_up(d, p, d).wait_recv())
        if d < UP[p]:
            pl.when(up_on(d + 1, z + 1, p))(lambda: ag_up(d + 1, p, d).start())
        if d <= DOWN[p]:
            pl.when(dn_on(d, z, p))(lambda: ag_dn(d, p, d).wait_recv())
        if d < DOWN[p]:
            pl.when(dn_on(d + 1, z - 1, p))(lambda: ag_dn(d + 1, p, d).start())

    def step(d, p, reach, is_on, step_out, buf, y, away, early):
        comes = is_on(d + 1, z + away, p) if d < reach else None
        if early:
            go = is_on(d, z, p)
            if comes is not None:
                go = jnp.logical_and(go, jnp.logical_not(comes))
            pl.when(go)(lambda: step_out(d, p).start())
        elif comes is not None:
            @pl.when(comes)
            def _():
                step_out(d + 1, p).wait_recv()
                part[y, p] += buf[d, p]
                step_out(d, p).start()

    def dn(d, p, early):
        if d == 1:
            if not early:
                home(p, False)
            return
        step(d, p, UP[p], up_on, rs_dn, dn_buf, wrap(z - d), 1, early)

    def up(e, p, early):
        step(e, p, DOWN[p], dn_on, rs_up, up_buf, wrap(z + e), -1, early)

    moves = {'ag': ag_step, 'dn': dn, 'up': up}

    def late(t):
        for name, *args in SCHEDULE.get(t, ()):
            moves[name](*args)

    local = [
        pltpu.make_async_copy(k_hbm, kv_all.at[z, 0], load_sem.at[0]),
        pltpu.make_async_copy(v_hbm, kv_all.at[z, 1], load_sem.at[1]),
        pltpu.make_async_copy(do_hbm, do_all.at[pl.ds(0, rows)], load_sem.at[2]),
        pltpu.make_async_copy(out_hbm, fwd, load_sem.at[3]),
        pltpu.make_async_copy(q_hbm, q_all.at[pl.ds(0, rows)], load_sem.at[4]),
    ]
    for c in local:
        c.start()

    barrier = pltpu.get_barrier_semaphore()
    for peer in (above, below, sibling):
        pl.semaphore_signal(barrier, inc=1, device_id=peer, device_id_type=MESH)
    pl.semaphore_wait(barrier, 3)

    for p in range(2):
        local[p].wait()
        pl.when(up_on(1, z + 1, p))(lambda: ag_up(1, p, 0).start())
        pl.when(dn_on(1, z - 1, p))(lambda: ag_dn(1, p, 0).start())
    for g in range(halves):
        for i in range(2):
            swap(i, g).start()

    @pl.when(core == 0)
    def _():
        for p in range(2):
            cross_kv(p).start()

    def widen(x, dst, base):
        for t in range(128):
            dst[pl.ds(pl.multiple_of(base + t * heads, heads), heads), :] = jnp.broadcast_to(x[:, t:t + 1], (heads, 128))

    local[2].wait()
    local[3].wait()
    stats[0, 0] = lse_in[...] * LOG2E
    lane = lax.broadcasted_iota(jnp.int32, (heads, 128), 1)

    def own_stats(i, carry):
        at = pl.ds(pl.multiple_of(i * 128, 128), 128)
        base = i * (128 * heads)
        r = pl.ds(pl.multiple_of(base, 128 * heads), 128 * heads)
        d = jnp.sum(do_all[r, :].astype(F32) * fwd[r, :].astype(F32), axis=-1, keepdims=True)
        wide = jnp.broadcast_to(d, (128 * heads, 128))
        dl_all[r, :] = wide
        dense = jnp.zeros((heads, 128), F32)
        for t in range(128):
            dense = jnp.where(lane == t, wide[t * heads:(t + 1) * heads], dense)
        stats[0, 1, :, at] = dense
        widen(stats[0, 0, :, at], lse_all, base)
        return carry

    lax.fori_loop(0, cols // 128, own_stats, 0)
    local[4].wait()
    part[...] = jnp.zeros_like(part)
    dq_all[...] = jnp.zeros_like(dq_all)
    swap_stats().start()

    def tiles(y, base, units, width, mask_from, c0=0):
        at = pl.ds(c0, width)
        k = kv_all[y, 0, at]
        v = kv_all[y, 1, at]
        ps, dss = [], []
        for u in range(units):
            r = pl.ds(pl.multiple_of(base + u * CHUNK, CHUNK), CHUNK)
            s = dot_nt(q_all[r, :], k)
            dp = dot_nt(do_all[r, :], v)
            p = jnp.exp2(s * (scale * LOG2E) - jnp.tile(lse_all[r, :], (1, width // 128)))
            if mask_from is not None:
                row = lax.broadcasted_iota(jnp.int32, p.shape, 0) + u * CHUNK
                col = lax.broadcasted_iota(jnp.int32, p.shape, 1) * heads - mask_from
                p = jnp.where(col <= row, p, 0.0)
            dss.append((p * (dp - jnp.tile(dl_all[r, :], (1, width // 128)))).astype(BF16))
            ps.append(p.astype(BF16))
        r = pl.ds(pl.multiple_of(base, CHUNK), CHUNK * units)
        ds = jnp.concatenate(dss, 0)
        part[y, 1, :, at] += dot_tn(do_all[r, :], jnp.concatenate(ps, 0))
        part[y, 0, :, at] += dot_tn(q_all[r, :], ds)
        dq_all[r, :] += dot_nn(ds, k)

    pairs = rows // (2 * CHUNK)

    def diag(width, i, carry):
        base = i * (2 * CHUNK)
        tiles(z, base, 2, width, base)
        return carry

    late(-2)
    lax.fori_loop(0, pairs // 2, functools.partial(diag, cols // 2), 0)
    late(-1)
    swap_stats().wait_recv()

    def sibling_stats(i, carry):
        at = pl.ds(pl.multiple_of(i * 128, 128), 128)
        base = rows + i * (128 * heads)
        widen(stats[1, 0, :, at], lse_all, base)
        widen(stats[1, 1, :, at], dl_all, base)
        return carry

    lax.fori_loop(0, cols // 128, sibling_stats, 0)

    def swap_wait():
        for g in range(halves):
            for i in range(2):
                swap(i, g).wait_recv()

    full = 4 * (len(OFFSETS) - 1)
    end = full + 8

    def rows_of(j):
        return (1 - j // 2) * rows + (j % 2) * GROUP

    def sweep(t, carry):
        for at in SCHEDULE:
            if 0 <= at < full:
                pl.when(t == at)(lambda: late(at))
        off = sum(jnp.where(t // 4 == i, o, 0) for i, o in enumerate(OFFSETS[:-1]))
        y = wrap(z + off)

        @pl.when(need(z, y))
        def _():
            tiles(y, rows_of(t % 4), UNIT, cols, None)
        return carry

    def sweep_half(h, t, carry):
        for at in SCHEDULE:
            if full + 4 * h <= at < full + 4 * h + 4:
                pl.when(t == at)(lambda: late(at))
        y = wrap(z + OFFSETS[-1])

        @pl.when(need(z, y))
        def _():
            tiles(y, rows_of(t % 4), UNIT, cols // 2, None, h * (cols // 2))
        return carry

    swap_wait()
    lax.fori_loop(0, full, sweep, 0)
    for h in range(2):
        lax.fori_loop(full + 4 * h, full + 4 * h + 4, functools.partial(sweep_half, h), 0)
        home(h, True)
    late(end)

    @pl.when(core == 1)
    def _():
        for p in range(2):
            cross_kv(p).wait_recv()

    crossed = jnp.where(core == 0, z, chips)
    tiles(crossed, rows_of(jnp.where(core == 0, 0, 3)), UNIT, cols, None)
    dq_swap().start()
    pl.when(core == 1)(lambda: cross_sum().start())
    late(end + 1)
    lax.fori_loop(pairs // 2, pairs, functools.partial(diag, cols), 0)
    late(end + 2)

    dq_swap().wait_recv()
    for g in range(rows // CHUNK):
        r = pl.ds(g * CHUNK, CHUNK)
        dq_out[r, :] = ((dq_all[r, :] + dq_in[r, :]) * scale).astype(BF16)

    @pl.when(core == 0)
    def _():
        cross_sum().wait_recv()
        part[z] += cross[...]

    for p in range(2):
        @pl.when(up_on(1, z + 1, p))
        def _():
            for h in range(2):
                rs_home(p, h).wait_recv()
            part[z, p] += dn_buf[0, p]

        @pl.when(dn_on(1, z - 1, p))
        def _():
            rs_up(1, p).wait_recv()
            part[z, p] += up_buf[0, p]

    dk_out[...] = (part[z, 0] * scale).T.astype(BF16)
    dv_out[...] = part[z, 1].T.astype(BF16)

    for g in range(halves):
        for i in range(2):
            swap(i, g).wait_send()
    swap_stats().wait_send()

    @pl.when(core == 0)
    def _():
        for p in range(2):
            cross_kv(p).wait_send()

    pl.when(core == 1)(lambda: cross_sum().wait_send())
    for p in range(2):
        for d in range(1, UP[p] + 1):
            pl.when(up_on(d, z + 1, p))(lambda: ag_up(d, p, d - 1).wait_send())
            if d > 1:
                pl.when(up_on(d, z, p))(lambda: rs_dn(d, p).wait_send())
        for h in range(2):
            pl.when(up_on(1, z, p))(lambda: rs_home(p, h).wait_send())
        for e in range(1, DOWN[p] + 1):
            pl.when(dn_on(e, z - 1, p))(lambda: ag_dn(e, p, e - 1).wait_send())
            pl.when(dn_on(e, z, p))(lambda: rs_up(e, p).wait_send())
    dq_swap().wait_send()


def deliver(dq, dk, dv, dq_out, dk_out, dv_out, a, b, c, sem_in, sem_out):
    pieces = 4
    step = dq.shape[0] // pieces
    moves = [(dk, b, dk_out), (dv, c, dv_out)] + [tuple(x.at[pl.ds(i * step, step)] for x in (dq, a, dq_out)) for i in range(pieces)]
    ins = [pltpu.make_async_copy(s, m, sem_in.at[i]) for i, (s, m, _) in enumerate(moves)]
    outs = [pltpu.make_async_copy(m, d, sem_out.at[i]) for i, (_, m, d) in enumerate(moves)]
    for x in ins:
        x.start()
    for x, o in zip(ins, outs):
        x.wait()
        o.start()
    for o in outs:
        o.wait()


def solution(mesh):
    n = mesh.shape['cp']
    row_spec = P(('dp', 'cp'))

    def local_fn(q_tok, k_tok, v_tok, fwd_out, d_out, lse_row):
        toks, heads, dim = q_tok.shape
        rows = toks * heads
        scale = dim ** -0.5
        flat = lambda x: x.reshape(rows, dim)
        chips = n // 2
        halves = rows // GROUP
        dma = pltpu.SemaphoreType.DMA
        hbm, vmem = pl.BlockSpec(memory_space=pl.ANY), pl.BlockSpec(memory_space=pltpu.VMEM)
        shapes = (jax.ShapeDtypeStruct((rows, dim), BF16), jax.ShapeDtypeStruct((toks, dim), BF16), jax.ShapeDtypeStruct((toks, dim), BF16))
        hops = dma((FAR, 2))
        grads = pl.pallas_call(
            functools.partial(kernel, n, scale),
            out_shape=shapes,
            in_specs=[hbm] * 5 + [vmem],
            out_specs=[vmem] * 3,
            scratch_shapes=[
                pltpu.VMEM((2 * rows, dim), BF16),
                pltpu.VMEM((2 * rows, dim), BF16),
                pltpu.VMEM((rows, dim), BF16),
                pltpu.VMEM((2 * rows, 128), F32),
                pltpu.VMEM((2 * rows, 128), F32),
                pltpu.VMEM((2, 2, heads, toks), F32),
                pltpu.VMEM((chips + 1, 2, toks, dim), BF16),
                pltpu.VMEM((chips + 1, 2, dim, toks), F32),
                pltpu.VMEM((2, dim, toks), F32),
                pltpu.VMEM((2 * rows, dim), F32),
                pltpu.VMEM((rows, dim), F32),
                pltpu.VMEM((FAR, 2, dim, toks), F32),
                pltpu.VMEM((FAR, 2, dim, toks), F32),
                dma((5,)), dma((3, halves)), dma((3, halves)),
                hops, hops, hops, hops, hops, hops, hops, hops,
                dma, dma, dma((3,)), dma((3,)), dma((2, 2)), dma((2, 2)),
            ],
            compiler_params=pltpu.CompilerParams(collective_id=0, has_side_effects=True, vmem_limit_bytes=60 * 2 ** 20),
        )(flat(q_tok), k_tok, v_tok, flat(fwd_out), flat(d_out), lse_row.T)
        dq, dk, dv = pl.pallas_call(
            deliver,
            out_shape=shapes,
            in_specs=[hbm] * 3,
            out_specs=[hbm] * 3,
            scratch_shapes=[pltpu.VMEM(s.shape, s.dtype) for s in shapes] + [dma((6,)), dma((6,))],
        )(*grads)
        return dq.reshape(q_tok.shape), dk, dv

    return jax.shard_map(local_fn, mesh=mesh, in_specs=(row_spec,) * 6, out_specs=(row_spec,) * 3, check_vma=False)
```

```python
import functools

import jax
import jax.numpy as jnp
from jax import lax
from jax.experimental import pallas as pl
from jax.experimental.pallas import tpu as pltpu
from jax.sharding import PartitionSpec as P

MESH = pl.DeviceIdType.MESH
HELP_AT = 10
LENT = 3
LOG2E = 1.4426950408889634
F32, BF16 = jnp.float32, jnp.bfloat16
CHUNK = 512
UNIT = 4
GROUP = CHUNK * UNIT
UP, DOWN = (4, 3), (3, 4)
FAR = 4
OFFSETS = (-2, -3, -4, 3, 1, 2, -1)
SCHEDULE = {
    -2: (('ag', 1, 0),),
    -1: (('ag', 1, 1),),
    0: (('ag', 2, 0), ('ag', 2, 1),),
    4: (('ag', 3, 0), ('ag', 3, 1),),
    6: (('dn', 2, 0, True),),
    7: (('ag', 4, 0),),
    8: (('ag', 4, 1),),
    9: (('dn', 3, 1, True),),
    12: (('up', 4, 1, True), ('dn', 4, 0, True),),
    14: (('dn', 3, 0, True), ('dn', 2, 1, False),),
    16: (('up', 3, 0, True),),
    17: (('dn', 3, 0, False),),
    18: (('up', 3, 1, False),),
    23: (('dn', 2, 0, False),),
    24: (('dn', 2, 1, True), ('up', 2, 0, False),),
    25: (('up', 3, 1, True),),
    27: (('up', 1, 0, True),),
    28: (('up', 2, 1, False),),
    29: (('dn', 1, 0, False), ('up', 2, 1, True),),
    32: (('up', 1, 0, False), ('dn', 1, 1, False), ('dn', 1, 0, True), ('dn', 1, 1, True),),
    33: (('up', 2, 0, True), ('up', 1, 1, False),),
    34: (('up', 1, 1, True),),
}


def dot_nt(a, b):
    return lax.dot_general(a, b, (((1,), (1,)), ((), ())), preferred_element_type=F32)


def dot_tn(a, b):
    return lax.dot_general(a, b, (((0,), (0,)), ((), ())), preferred_element_type=F32)


def dot_nn(a, b):
    return jnp.dot(a, b, preferred_element_type=F32)


def kernel(n, scale, q_hbm, k_hbm, v_hbm, out_hbm, do_hbm, lse_in, dq_out, dk_out, dv_out,
           q_all, do_all, fwd, lse_all, dl_all, stats, kv_all, part, cross, dq_all, lent_dq, dq_in, up_buf, dn_buf,
           load_sem, xs_sem, xr_sem, agu_s, agu_r, agd_s, agd_r, rsd_s, rsd_r, rsu_s, rsu_r, dqs_sem, dqr_sem, cs_sem, cr_sem, home_s, home_r, lend_s, lend_r, pass_s, pass_r, back_s, back_r):
    chips = n // 2
    me = lax.axis_index('cp')
    z = me // 2
    core = me % 2
    rows = q_hbm.shape[0]
    halves = rows // GROUP
    cols, dim = k_hbm.shape
    heads = rows // cols
    wrap = lambda i: lax.rem(i + 2 * chips, chips)
    above = {'cp': 2 * wrap(z + 1) + core}
    below = {'cp': 2 * wrap(z - 1) + core}
    sibling = {'cp': 2 * z + 1 - core}

    def need(chip, y):
        return wrap(y) < wrap(chip)

    def any_of(flags):
        return functools.reduce(jnp.logical_or, flags)

    def up_on(d, z0, p):
        return any_of([need(z0 + i, z0 - d) for i in range(UP[p] - d + 1)])

    def dn_on(e, z0, p):
        return any_of([need(z0 - i, z0 + e) for i in range(DOWN[p] - e + 1)])

    def remote(src, dst, ss, rs, to):
        return pltpu.make_async_remote_copy(src_ref=src, dst_ref=dst, send_sem=ss, recv_sem=rs, device_id=to, device_id_type=MESH)

    def ag_up(d, p, dist):
        blk = kv_all.at[wrap(z - dist), p]
        return remote(blk, blk, agu_s.at[d - 1, p], agu_r.at[d - 1, p], above)

    def ag_dn(e, p, dist):
        blk = kv_all.at[wrap(z + dist), p]
        return remote(blk, blk, agd_s.at[e - 1, p], agd_r.at[e - 1, p], below)

    def rs_dn(d, p):
        return remote(part.at[wrap(z - d), p], dn_buf.at[d - 1, p], rsd_s.at[d - 1, p], rsd_r.at[d - 1, p], below)

    def rs_home(p, h):
        at = pl.ds(h * (cols // 2), cols // 2)
        return remote(part.at[wrap(z - 1), p, :, at], dn_buf.at[0, p, :, at], home_s.at[p, h], home_r.at[p, h], below)

    def home(h, early):
        comes = up_on(2, z + 1, 0)
        go = jnp.logical_and(up_on(1, z, 0), jnp.logical_not(comes)) if early else comes

        @pl.when(go)
        def _():
            for p in range(2):
                if not early and h == 0:
                    rs_dn(2, p).wait_recv()
                    part[wrap(z - 1), p] += dn_buf[1, p]
                rs_home(p, h).start()

    def rs_up(e, p):
        return remote(part.at[wrap(z + e), p], up_buf.at[e - 1, p], rsu_s.at[e - 1, p], rsu_r.at[e - 1, p], above)

    def swap(i, g):
        src, dst = ((q_hbm, q_all), (do_hbm, do_all))[i]
        return remote(src.at[pl.ds(g * GROUP, GROUP)], dst.at[pl.ds(rows + g * GROUP, GROUP)], xs_sem.at[i, g], xr_sem.at[i, g], sibling)

    def swap_stats():
        return remote(stats.at[0], stats.at[1], xs_sem.at[2, 0], xr_sem.at[2, 0], sibling)

    def cross_kv(p):
        return remote((k_hbm, v_hbm)[p], kv_all.at[chips, p], cs_sem.at[p], cr_sem.at[p], sibling)

    def cross_sum():
        return remote(part.at[chips], cross, cs_sem.at[2], cr_sem.at[2], sibling)

    lender, helper = z == chips - 1, z == 0
    theirs = pl.ds(2 * rows, GROUP)
    theirs_too = pl.ds(2 * rows + GROUP, GROUP)

    def lend(i):
        half = pl.ds(rows - GROUP, GROUP)
        src = (q_hbm.at[half], do_hbm.at[half], stats.at[0])[i]
        dst = (q_all.at[theirs], do_all.at[theirs], stats.at[2])[i]
        return remote(src, dst, lend_s.at[i], lend_r.at[i], above)

    def pass_on(i):
        src = (q_all.at[theirs], do_all.at[theirs], stats.at[2])[i]
        dst = (q_all.at[theirs_too], do_all.at[theirs_too], stats.at[3])[i]
        return remote(src, dst, pass_s.at[i], pass_r.at[i], sibling)

    def merge():
        return remote(dq_all.at[theirs_too], lent_dq, back_s.at[0], back_r.at[0], sibling)

    def give_back():
        return remote(dq_all.at[theirs], lent_dq, back_s.at[1], back_r.at[1], below)

    def dq_swap():
        return remote(dq_all.at[pl.ds(rows, rows)], dq_in, dqs_sem, dqr_sem, sibling)

    def ag_step(d, p):
        if d <= UP[p]:
            pl.when(up_on(d, z, p))(lambda: ag_up(d, p, d).wait_recv())
        if d < UP[p]:
            pl.when(up_on(d + 1, z + 1, p))(lambda: ag_up(d + 1, p, d).start())
        if d <= DOWN[p]:
            pl.when(dn_on(d, z, p))(lambda: ag_dn(d, p, d).wait_recv())
        if d < DOWN[p]:
            pl.when(dn_on(d + 1, z - 1, p))(lambda: ag_dn(d + 1, p, d).start())

    def step(d, p, reach, is_on, step_out, buf, y, away, early):
        comes = is_on(d + 1, z + away, p) if d < reach else None
        if early:
            go = is_on(d, z, p)
            if comes is not None:
                go = jnp.logical_and(go, jnp.logical_not(comes))
            pl.when(go)(lambda: step_out(d, p).start())
        elif comes is not None:
            @pl.when(comes)
            def _():
                step_out(d + 1, p).wait_recv()
                part[y, p] += buf[d, p]
                step_out(d, p).start()

    def dn(d, p, early):
        if d == 1:
            if not early:
                home(p, False)
            return
        step(d, p, UP[p], up_on, rs_dn, dn_buf, wrap(z - d), 1, early)

    def up(e, p, early):
        step(e, p, DOWN[p], dn_on, rs_up, up_buf, wrap(z + e), -1, early)

    moves = {'ag': ag_step, 'dn': dn, 'up': up}

    def late(t):
        for name, *args in SCHEDULE.get(t, ()):
            moves[name](*args)

    local = [
        pltpu.make_async_copy(k_hbm, kv_all.at[z, 0], load_sem.at[0]),
        pltpu.make_async_copy(v_hbm, kv_all.at[z, 1], load_sem.at[1]),
        pltpu.make_async_copy(do_hbm, do_all.at[pl.ds(0, rows)], load_sem.at[2]),
        pltpu.make_async_copy(out_hbm, fwd, load_sem.at[3]),
        pltpu.make_async_copy(q_hbm, q_all.at[pl.ds(0, rows)], load_sem.at[4]),
    ]
    for c in local:
        c.start()

    barrier = pltpu.get_barrier_semaphore()
    for peer in (above, below, sibling):
        pl.semaphore_signal(barrier, inc=1, device_id=peer, device_id_type=MESH)
    pl.semaphore_wait(barrier, 3)

    for p in range(2):
        local[p].wait()
        pl.when(up_on(1, z + 1, p))(lambda: ag_up(1, p, 0).start())
        pl.when(dn_on(1, z - 1, p))(lambda: ag_dn(1, p, 0).start())
    for g in range(halves):
        for i in range(2):
            swap(i, g).start()

    @pl.when(core == 0)
    def _():
        for p in range(2):
            cross_kv(p).start()

    @pl.when(lender)
    def _():
        for i in range(2):
            lend(i).start()

    def widen(x, dst, base):
        for t in range(128):
            dst[pl.ds(pl.multiple_of(base + t * heads, heads), heads), :] = jnp.broadcast_to(x[:, t:t + 1], (heads, 128))

    local[2].wait()
    local[3].wait()
    stats[0, 0] = lse_in[...] * LOG2E
    lane = lax.broadcasted_iota(jnp.int32, (heads, 128), 1)

    def own_stats(i, carry):
        at = pl.ds(pl.multiple_of(i * 128, 128), 128)
        base = i * (128 * heads)
        r = pl.ds(pl.multiple_of(base, 128 * heads), 128 * heads)
        d = jnp.sum(do_all[r, :].astype(F32) * fwd[r, :].astype(F32), axis=-1, keepdims=True)
        wide = jnp.broadcast_to(d, (128 * heads, 128))
        dl_all[r, :] = wide
        dense = jnp.zeros((heads, 128), F32)
        for t in range(128):
            dense = jnp.where(lane == t, wide[t * heads:(t + 1) * heads], dense)
        stats[0, 1, :, at] = dense
        widen(stats[0, 0, :, at], lse_all, base)
        return carry

    lax.fori_loop(0, cols // 128, own_stats, 0)
    local[4].wait()
    part[...] = jnp.zeros_like(part)
    dq_all[...] = jnp.zeros_like(dq_all)
    swap_stats().start()
    pl.when(lender)(lambda: lend(2).start())

    def tiles(y, base, units, width, mask_from, c0=0):
        at = pl.ds(c0, width)
        k = kv_all[y, 0, at]
        v = kv_all[y, 1, at]
        ps, dss = [], []
        for u in range(units):
            r = pl.ds(pl.multiple_of(base + u * CHUNK, CHUNK), CHUNK)
            s = dot_nt(q_all[r, :], k)
            dp = dot_nt(do_all[r, :], v)
            p = jnp.exp2(s * (scale * LOG2E) - jnp.tile(lse_all[r, :], (1, width // 128)))
            if mask_from is not None:
                row = lax.broadcasted_iota(jnp.int32, p.shape, 0) + u * CHUNK
                col = lax.broadcasted_iota(jnp.int32, p.shape, 1) * heads - mask_from
                p = jnp.where(col <= row, p, 0.0)
            dss.append((p * (dp - jnp.tile(dl_all[r, :], (1, width // 128)))).astype(BF16))
            ps.append(p.astype(BF16))
        r = pl.ds(pl.multiple_of(base, CHUNK), CHUNK * units)
        ds = jnp.concatenate(dss, 0)
        part[y, 1, :, at] += dot_tn(do_all[r, :], jnp.concatenate(ps, 0))
        part[y, 0, :, at] += dot_tn(q_all[r, :], ds)
        dq_all[r, :] += dot_nn(ds, k)

    pairs = rows // (2 * CHUNK)

    def diag(width, i, carry):
        base = i * (2 * CHUNK)
        tiles(z, base, 2, width, base)
        return carry

    late(-2)
    lax.fori_loop(0, pairs // 2, functools.partial(diag, cols // 2), 0)
    late(-1)
    swap_stats().wait_recv()

    def sibling_stats(i, carry):
        at = pl.ds(pl.multiple_of(i * 128, 128), 128)
        base = rows + i * (128 * heads)
        widen(stats[1, 0, :, at], lse_all, base)
        widen(stats[1, 1, :, at], dl_all, base)
        return carry

    lax.fori_loop(0, cols // 128, sibling_stats, 0)

    def swap_wait():
        for g in range(halves):
            for i in range(2):
                swap(i, g).wait_recv()

    full = 4 * (len(OFFSETS) - 1)
    end = full + 8

    def help_out():
        for i in range(3):
            lend(i).wait_recv()
            pass_on(i).start()
        first = (rows - GROUP) // heads

        def widen_lent(b, carry):
            at = pl.ds(pl.multiple_of(first + b * 128, 128), 128)
            base = 2 * rows + b * (128 * heads)
            widen(stats[2, 0, :, at], lse_all, base)
            widen(stats[2, 1, :, at], dl_all, base)
            return carry

        def widen_passed(b, carry):
            at = pl.ds(pl.multiple_of(first + b * 128, 128), 128)
            base = 2 * rows + GROUP + b * (128 * heads)
            widen(stats[3, 0, :, at], lse_all, base)
            widen(stats[3, 1, :, at], dl_all, base)
            return carry

        blocks = GROUP // (128 * heads)
        lax.fori_loop(0, blocks, widen_lent, 0)
        for i in range(3):
            pass_on(i).wait_recv()
        lax.fori_loop(0, blocks, widen_passed, 0)

        def pieces(i, carry):
            tiles(i % LENT, 2 * rows + (1 - i // LENT) * GROUP, UNIT, cols, None)
            return carry

        lax.fori_loop(0, LENT, pieces, 0)
        merge().start()
        lax.fori_loop(LENT, 2 * LENT, pieces, 0)
        merge().wait_recv()
        dq_all[theirs, :] += lent_dq[...]
        give_back().start()

    def rows_of(j):
        return (1 - j // 2) * rows + (j % 2) * GROUP

    def sweep(t, carry):
        for at in SCHEDULE:
            if 0 <= at < full:
                pl.when(t == at)(lambda: late(at))
        pl.when(jnp.logical_and(helper, t == HELP_AT))(help_out)
        off = sum(jnp.where(t // 4 == i, o, 0) for i, o in enumerate(OFFSETS[:-1]))
        y = wrap(z + off)

        lent = jnp.logical_and(lender, jnp.logical_and(y < LENT, t % 2 == 1))

        @pl.when(jnp.logical_and(need(z, y), jnp.logical_not(lent)))
        def _():
            tiles(y, rows_of(t % 4), UNIT, cols, None)
        return carry

    def sweep_half(h, t, carry):
        for at in SCHEDULE:
            if full + 4 * h <= at < full + 4 * h + 4:
                pl.when(t == at)(lambda: late(at))
        y = wrap(z + OFFSETS[-1])

        @pl.when(need(z, y))
        def _():
            tiles(y, rows_of(t % 4), UNIT, cols // 2, None, h * (cols // 2))
        return carry

    swap_wait()
    lax.fori_loop(0, full, sweep, 0)
    for h in range(2):
        lax.fori_loop(full + 4 * h, full + 4 * h + 4, functools.partial(sweep_half, h), 0)
        home(h, True)
    late(end)

    @pl.when(core == 1)
    def _():
        for p in range(2):
            cross_kv(p).wait_recv()

    crossed = jnp.where(core == 0, z, chips)
    tiles(crossed, rows_of(jnp.where(core == 0, 0, 3)), UNIT, cols, None)
    dq_swap().start()
    pl.when(core == 1)(lambda: cross_sum().start())
    late(end + 1)
    lax.fori_loop(pairs // 2, pairs, functools.partial(diag, cols), 0)
    late(end + 2)

    @pl.when(lender)
    def _():
        give_back().wait_recv()
        r = pl.ds(rows - GROUP, GROUP)
        dq_all[r, :] += lent_dq[...]

    dq_swap().wait_recv()
    for g in range(rows // CHUNK):
        r = pl.ds(g * CHUNK, CHUNK)
        dq_out[r, :] = ((dq_all[r, :] + dq_in[r, :]) * scale).astype(BF16)

    @pl.when(core == 0)
    def _():
        cross_sum().wait_recv()
        part[z] += cross[...]

    for p in range(2):
        @pl.when(up_on(1, z + 1, p))
        def _():
            for h in range(2):
                rs_home(p, h).wait_recv()
            part[z, p] += dn_buf[0, p]

        @pl.when(dn_on(1, z - 1, p))
        def _():
            rs_up(1, p).wait_recv()
            part[z, p] += up_buf[0, p]

    dk_out[...] = (part[z, 0] * scale).T.astype(BF16)
    dv_out[...] = part[z, 1].T.astype(BF16)

    for g in range(halves):
        for i in range(2):
            swap(i, g).wait_send()
    swap_stats().wait_send()

    @pl.when(core == 0)
    def _():
        for p in range(2):
            cross_kv(p).wait_send()

    pl.when(core == 1)(lambda: cross_sum().wait_send())
    for p in range(2):
        for d in range(1, UP[p] + 1):
            pl.when(up_on(d, z + 1, p))(lambda: ag_up(d, p, d - 1).wait_send())
            if d > 1:
                pl.when(up_on(d, z, p))(lambda: rs_dn(d, p).wait_send())
        for h in range(2):
            pl.when(up_on(1, z, p))(lambda: rs_home(p, h).wait_send())
        for e in range(1, DOWN[p] + 1):
            pl.when(dn_on(e, z - 1, p))(lambda: ag_dn(e, p, e - 1).wait_send())
            pl.when(dn_on(e, z, p))(lambda: rs_up(e, p).wait_send())
    dq_swap().wait_send()

    @pl.when(lender)
    def _():
        for i in range(3):
            lend(i).wait_send()

    @pl.when(helper)
    def _():
        for i in range(3):
            pass_on(i).wait_send()
        merge().wait_send()
        give_back().wait_send()


def deliver(dq, dk, dv, dq_out, dk_out, dv_out, a, b, c, sem_in, sem_out):
    pieces = 4
    step = dq.shape[0] // pieces
    moves = [(dk, b, dk_out), (dv, c, dv_out)] + [tuple(x.at[pl.ds(i * step, step)] for x in (dq, a, dq_out)) for i in range(pieces)]
    ins = [pltpu.make_async_copy(s, m, sem_in.at[i]) for i, (s, m, _) in enumerate(moves)]
    outs = [pltpu.make_async_copy(m, d, sem_out.at[i]) for i, (_, m, d) in enumerate(moves)]
    for x in ins:
        x.start()
    for x, o in zip(ins, outs):
        x.wait()
        o.start()
    for o in outs:
        o.wait()


def solution(mesh):
    n = mesh.shape['cp']
    row_spec = P(('dp', 'cp'))

    def local_fn(q_tok, k_tok, v_tok, fwd_out, d_out, lse_row):
        toks, heads, dim = q_tok.shape
        rows = toks * heads
        scale = dim ** -0.5
        flat = lambda x: x.reshape(rows, dim)
        chips = n // 2
        halves = rows // GROUP
        held = 2 * rows + 2 * GROUP
        dma = pltpu.SemaphoreType.DMA
        hbm, vmem = pl.BlockSpec(memory_space=pl.ANY), pl.BlockSpec(memory_space=pltpu.VMEM)
        shapes = (jax.ShapeDtypeStruct((rows, dim), BF16), jax.ShapeDtypeStruct((toks, dim), BF16), jax.ShapeDtypeStruct((toks, dim), BF16))
        hops = dma((FAR, 2))
        grads = pl.pallas_call(
            functools.partial(kernel, n, scale),
            out_shape=shapes,
            in_specs=[hbm] * 5 + [vmem],
            out_specs=[vmem] * 3,
            scratch_shapes=[
                pltpu.VMEM((held, dim), BF16),
                pltpu.VMEM((held, dim), BF16),
                pltpu.VMEM((rows, dim), BF16),
                pltpu.VMEM((held, 128), F32),
                pltpu.VMEM((held, 128), F32),
                pltpu.VMEM((4, 2, heads, toks), F32),
                pltpu.VMEM((chips + 1, 2, toks, dim), BF16),
                pltpu.VMEM((chips + 1, 2, dim, toks), F32),
                pltpu.VMEM((2, dim, toks), F32),
                pltpu.VMEM((held, dim), F32),
                pltpu.VMEM((GROUP, dim), F32),
                pltpu.VMEM((rows, dim), F32),
                pltpu.VMEM((FAR, 2, dim, toks), F32),
                pltpu.VMEM((FAR, 2, dim, toks), F32),
                dma((5,)), dma((3, halves)), dma((3, halves)),
                hops, hops, hops, hops, hops, hops, hops, hops,
                dma, dma, dma((3,)), dma((3,)), dma((2, 2)), dma((2, 2)),
                dma((3,)), dma((3,)), dma((3,)), dma((3,)), dma((2,)), dma((2,)),
            ],
            compiler_params=pltpu.CompilerParams(collective_id=0, has_side_effects=True, vmem_limit_bytes=60 * 2 ** 20),
        )(flat(q_tok), k_tok, v_tok, flat(fwd_out), flat(d_out), lse_row.T)
        dq, dk, dv = pl.pallas_call(
            deliver,
            out_shape=shapes,
            in_specs=[hbm] * 3,
            out_specs=[hbm] * 3,
            scratch_shapes=[pltpu.VMEM(s.shape, s.dtype) for s in shapes] + [dma((6,)), dma((6,))],
        )(*grads)
        return dq.reshape(q_tok.shape), dk, dv

    return jax.shard_map(local_fn, mesh=mesh, in_specs=(row_spec,) * 6, out_specs=(row_spec,) * 3, check_vma=False)
```

```python
import functools

import jax
import jax.numpy as jnp
from jax import lax
from jax.experimental import pallas as pl
from jax.experimental.pallas import tpu as pltpu
from jax.sharding import PartitionSpec as P

MESH = pl.DeviceIdType.MESH
HELP_AT = 10
LENT = 3
LOG2E = 1.4426950408889634
F32, BF16 = jnp.float32, jnp.bfloat16
CHUNK = 512
UNIT = 4
GROUP = CHUNK * UNIT
UP, DOWN = (4, 3), (3, 4)
FAR = 4
OFFSETS = (-2, -3, -4, 3, 1, 2, -1)
SCHEDULE = {
    -2: (('ag', 1, 0), ('ag', 1, 1),),
    0: (('ag', 2, 0), ('ag', 2, 1),),
    3: (('ag', 3, 0), ('ag', 3, 1),),
    6: (('ag', 4, 1),),
    8: (('ag', 4, 0), ('dn', 3, 1, True),),
    12: (('up', 4, 1, True), ('dn', 4, 0, True), ('dn', 3, 0, True),),
    15: (('dn', 2, 0, True),),
    16: (('up', 3, 0, True),),
    18: (('dn', 3, 0, False),),
    19: (('up', 3, 1, False),),
    20: (('dn', 2, 1, False),),
    23: (('dn', 2, 1, True),),
    24: (('dn', 2, 0, False), ('up', 2, 0, False),),
    27: (('up', 2, 1, False),),
    28: (('dn', 1, 0, False),),
    30: (('up', 2, 1, True), ('up', 1, 0, False),),
    31: (('up', 2, 0, True),),
    32: (('up', 3, 1, True), ('dn', 1, 0, True), ('dn', 1, 1, False),),
    33: (('up', 1, 1, False), ('dn', 1, 1, True),),
    34: (('up', 1, 1, True), ('up', 1, 0, True),),
}


def dot_nt(a, b):
    return lax.dot_general(a, b, (((1,), (1,)), ((), ())), preferred_element_type=F32)


def dot_tn(a, b):
    return lax.dot_general(a, b, (((0,), (0,)), ((), ())), preferred_element_type=F32)


def dot_nn(a, b):
    return jnp.dot(a, b, preferred_element_type=F32)


def kernel(n, scale, q_hbm, k_hbm, v_hbm, out_hbm, do_hbm, lse_in, dq_out, dk_out, dv_out,
           q_all, do_all, fwd, lse_all, dl_all, stats, kv_all, part, cross, dq_all, lent_dq, dq_in, up_buf, dn_buf,
           load_sem, xs_sem, xr_sem, agu_s, agu_r, agd_s, agd_r, rsd_s, rsd_r, rsu_s, rsu_r, dqs_sem, dqr_sem, cs_sem, cr_sem, home_s, home_r, lend_s, lend_r, pass_s, pass_r, back_s, back_r):
    chips = n // 2
    me = lax.axis_index('cp')
    z = me // 2
    core = me % 2
    rows = q_hbm.shape[0]
    halves = rows // GROUP
    cols, dim = k_hbm.shape
    heads = rows // cols
    wrap = lambda i: lax.rem(i + 2 * chips, chips)
    above = {'cp': 2 * wrap(z + 1) + core}
    below = {'cp': 2 * wrap(z - 1) + core}
    sibling = {'cp': 2 * z + 1 - core}

    def need(chip, y):
        return wrap(y) < wrap(chip)

    def any_of(flags):
        return functools.reduce(jnp.logical_or, flags)

    def up_on(d, z0, p):
        return any_of([need(z0 + i, z0 - d) for i in range(UP[p] - d + 1)])

    def dn_on(e, z0, p):
        return any_of([need(z0 - i, z0 + e) for i in range(DOWN[p] - e + 1)])

    def remote(src, dst, ss, rs, to):
        return pltpu.make_async_remote_copy(src_ref=src, dst_ref=dst, send_sem=ss, recv_sem=rs, device_id=to, device_id_type=MESH)

    def ag_up(d, p, dist):
        blk = kv_all.at[wrap(z - dist), p]
        return remote(blk, blk, agu_s.at[d - 1, p], agu_r.at[d - 1, p], above)

    def ag_dn(e, p, dist):
        blk = kv_all.at[wrap(z + dist), p]
        return remote(blk, blk, agd_s.at[e - 1, p], agd_r.at[e - 1, p], below)

    def rs_dn(d, p):
        return remote(part.at[wrap(z - d), p], dn_buf.at[d - 1, p], rsd_s.at[d - 1, p], rsd_r.at[d - 1, p], below)

    def rs_home(p, h):
        at = pl.ds(h * (cols // 2), cols // 2)
        return remote(part.at[wrap(z - 1), p, :, at], dn_buf.at[0, p, :, at], home_s.at[p, h], home_r.at[p, h], below)

    def home(h, early):
        comes = up_on(2, z + 1, 0)
        go = jnp.logical_and(up_on(1, z, 0), jnp.logical_not(comes)) if early else comes

        @pl.when(go)
        def _():
            for p in range(2):
                if not early and h == 0:
                    rs_dn(2, p).wait_recv()
                    part[wrap(z - 1), p] += dn_buf[1, p]
                rs_home(p, h).start()

    def rs_up(e, p):
        return remote(part.at[wrap(z + e), p], up_buf.at[e - 1, p], rsu_s.at[e - 1, p], rsu_r.at[e - 1, p], above)

    def swap(i, g):
        src, dst = ((q_hbm, q_all), (do_hbm, do_all))[i]
        return remote(src.at[pl.ds(g * GROUP, GROUP)], dst.at[pl.ds(rows + g * GROUP, GROUP)], xs_sem.at[i, g], xr_sem.at[i, g], sibling)

    def swap_stats():
        return remote(stats.at[0], stats.at[1], xs_sem.at[2, 0], xr_sem.at[2, 0], sibling)

    def cross_kv(p):
        return remote((k_hbm, v_hbm)[p], kv_all.at[chips, p], cs_sem.at[p], cr_sem.at[p], sibling)

    def cross_sum():
        return remote(part.at[chips], cross, cs_sem.at[2], cr_sem.at[2], sibling)

    lender, helper = z == chips - 1, z == 0
    theirs = pl.ds(2 * rows, GROUP)
    theirs_too = pl.ds(2 * rows + GROUP, GROUP)

    def lend(i):
        half = pl.ds(rows - GROUP, GROUP)
        src = (q_hbm.at[half], do_hbm.at[half], stats.at[0])[i]
        dst = (q_all.at[theirs], do_all.at[theirs], stats.at[2])[i]
        return remote(src, dst, lend_s.at[i], lend_r.at[i], above)

    def pass_on(i):
        src = (q_all.at[theirs], do_all.at[theirs], stats.at[2])[i]
        dst = (q_all.at[theirs_too], do_all.at[theirs_too], stats.at[3])[i]
        return remote(src, dst, pass_s.at[i], pass_r.at[i], sibling)

    def merge():
        return remote(dq_all.at[theirs_too], lent_dq, back_s.at[0], back_r.at[0], sibling)

    def give_back():
        return remote(dq_all.at[theirs], lent_dq, back_s.at[1], back_r.at[1], below)

    def dq_swap():
        return remote(dq_all.at[pl.ds(rows, rows)], dq_in, dqs_sem, dqr_sem, sibling)

    def ag_step(d, p):
        if d <= UP[p]:
            pl.when(up_on(d, z, p))(lambda: ag_up(d, p, d).wait_recv())
        if d < UP[p]:
            pl.when(up_on(d + 1, z + 1, p))(lambda: ag_up(d + 1, p, d).start())
        if d <= DOWN[p]:
            pl.when(dn_on(d, z, p))(lambda: ag_dn(d, p, d).wait_recv())
        if d < DOWN[p]:
            pl.when(dn_on(d + 1, z - 1, p))(lambda: ag_dn(d + 1, p, d).start())

    def step(d, p, reach, is_on, step_out, buf, y, away, early):
        comes = is_on(d + 1, z + away, p) if d < reach else None
        if early:
            go = is_on(d, z, p)
            if comes is not None:
                go = jnp.logical_and(go, jnp.logical_not(comes))
            pl.when(go)(lambda: step_out(d, p).start())
        elif comes is not None:
            @pl.when(comes)
            def _():
                step_out(d + 1, p).wait_recv()
                part[y, p] += buf[d, p]
                step_out(d, p).start()

    def dn(d, p, early):
        if d == 1:
            if not early:
                home(p, False)
            return
        step(d, p, UP[p], up_on, rs_dn, dn_buf, wrap(z - d), 1, early)

    def up(e, p, early):
        step(e, p, DOWN[p], dn_on, rs_up, up_buf, wrap(z + e), -1, early)

    moves = {'ag': ag_step, 'dn': dn, 'up': up}

    def late(t):
        for name, *args in SCHEDULE.get(t, ()):
            moves[name](*args)

    local = [
        pltpu.make_async_copy(k_hbm, kv_all.at[z, 0], load_sem.at[0]),
        pltpu.make_async_copy(v_hbm, kv_all.at[z, 1], load_sem.at[1]),
        pltpu.make_async_copy(do_hbm, do_all.at[pl.ds(0, rows)], load_sem.at[2]),
        pltpu.make_async_copy(out_hbm, fwd, load_sem.at[3]),
        pltpu.make_async_copy(q_hbm, q_all.at[pl.ds(0, rows)], load_sem.at[4]),
    ]
    for c in local:
        c.start()

    barrier = pltpu.get_barrier_semaphore()
    for peer in (above, below, sibling):
        pl.semaphore_signal(barrier, inc=1, device_id=peer, device_id_type=MESH)
    pl.semaphore_wait(barrier, 3)

    for p in range(2):
        local[p].wait()
        pl.when(up_on(1, z + 1, p))(lambda: ag_up(1, p, 0).start())
        pl.when(dn_on(1, z - 1, p))(lambda: ag_dn(1, p, 0).start())
    for g in range(halves):
        for i in range(2):
            swap(i, g).start()

    @pl.when(core == 0)
    def _():
        for p in range(2):
            cross_kv(p).start()

    @pl.when(lender)
    def _():
        for i in range(2):
            lend(i).start()

    def widen(x, dst, base):
        for t in range(128):
            dst[pl.ds(pl.multiple_of(base + t * heads, heads), heads), :] = jnp.broadcast_to(x[:, t:t + 1], (heads, 128))

    local[2].wait()
    local[3].wait()
    stats[0, 0] = lse_in[...] * LOG2E
    lane = lax.broadcasted_iota(jnp.int32, (heads, 128), 1)

    def own_stats(i, carry):
        at = pl.ds(pl.multiple_of(i * 128, 128), 128)
        base = i * (128 * heads)
        r = pl.ds(pl.multiple_of(base, 128 * heads), 128 * heads)
        d = jnp.sum(do_all[r, :].astype(F32) * fwd[r, :].astype(F32), axis=-1, keepdims=True)
        wide = jnp.broadcast_to(d, (128 * heads, 128))
        dl_all[r, :] = wide
        dense = jnp.zeros((heads, 128), F32)
        for t in range(128):
            dense = jnp.where(lane == t, wide[t * heads:(t + 1) * heads], dense)
        stats[0, 1, :, at] = dense
        widen(stats[0, 0, :, at], lse_all, base)
        return carry

    lax.fori_loop(0, cols // 128, own_stats, 0)
    local[4].wait()
    part[...] = jnp.zeros_like(part)
    dq_all[...] = jnp.zeros_like(dq_all)
    swap_stats().start()
    pl.when(lender)(lambda: lend(2).start())

    def tiles(y, base, units, width, mask_from, c0=0):
        at = pl.ds(c0, width)
        k = kv_all[y, 0, at]
        v = kv_all[y, 1, at]
        ps, dss = [], []
        for u in range(units):
            r = pl.ds(pl.multiple_of(base + u * CHUNK, CHUNK), CHUNK)
            s = dot_nt(q_all[r, :], k)
            dp = dot_nt(do_all[r, :], v)
            p = jnp.exp2(s * (scale * LOG2E) - jnp.tile(lse_all[r, :], (1, width // 128)))
            if mask_from is not None:
                row = lax.broadcasted_iota(jnp.int32, p.shape, 0) + u * CHUNK
                col = lax.broadcasted_iota(jnp.int32, p.shape, 1) * heads - mask_from
                p = jnp.where(col <= row, p, 0.0)
            dss.append((p * (dp - jnp.tile(dl_all[r, :], (1, width // 128)))).astype(BF16))
            ps.append(p.astype(BF16))
        r = pl.ds(pl.multiple_of(base, CHUNK), CHUNK * units)
        ds = jnp.concatenate(dss, 0)
        part[y, 1, :, at] += dot_tn(do_all[r, :], jnp.concatenate(ps, 0))
        part[y, 0, :, at] += dot_tn(q_all[r, :], ds)
        dq_all[r, :] += dot_nn(ds, k)

    pairs = rows // (2 * CHUNK)

    def diag(width, i, carry):
        base = i * (2 * CHUNK)
        tiles(z, base, 2, width, base)
        return carry

    late(-2)
    lax.fori_loop(0, pairs // 2, functools.partial(diag, cols // 2), 0)
    swap_stats().wait_recv()

    def sibling_stats(i, carry):
        at = pl.ds(pl.multiple_of(i * 128, 128), 128)
        base = rows + i * (128 * heads)
        widen(stats[1, 0, :, at], lse_all, base)
        widen(stats[1, 1, :, at], dl_all, base)
        return carry

    lax.fori_loop(0, cols // 128, sibling_stats, 0)

    def swap_wait():
        for g in range(halves):
            for i in range(2):
                swap(i, g).wait_recv()

    full = 4 * (len(OFFSETS) - 1)
    end = full + 8

    def help_out():
        for i in range(3):
            lend(i).wait_recv()
            pass_on(i).start()
        first = (rows - GROUP) // heads

        def widen_lent(b, carry):
            at = pl.ds(pl.multiple_of(first + b * 128, 128), 128)
            base = 2 * rows + b * (128 * heads)
            widen(stats[2, 0, :, at], lse_all, base)
            widen(stats[2, 1, :, at], dl_all, base)
            return carry

        def widen_passed(b, carry):
            at = pl.ds(pl.multiple_of(first + b * 128, 128), 128)
            base = 2 * rows + GROUP + b * (128 * heads)
            widen(stats[3, 0, :, at], lse_all, base)
            widen(stats[3, 1, :, at], dl_all, base)
            return carry

        blocks = GROUP // (128 * heads)
        lax.fori_loop(0, blocks, widen_lent, 0)
        for i in range(3):
            pass_on(i).wait_recv()
        lax.fori_loop(0, blocks, widen_passed, 0)

        def pieces(i, carry):
            tiles(i % LENT, 2 * rows + (1 - i // LENT) * GROUP, UNIT, cols, None)
            return carry

        lax.fori_loop(0, LENT, pieces, 0)
        merge().start()
        lax.fori_loop(LENT, 2 * LENT, pieces, 0)
        merge().wait_recv()
        dq_all[theirs, :] += lent_dq[...]
        give_back().start()

    def rows_of(j):
        return (1 - j // 2) * rows + (j % 2) * GROUP

    def sweep(t, carry):
        for at in SCHEDULE:
            if 0 <= at < full:
                pl.when(t == at)(lambda: late(at))
        pl.when(jnp.logical_and(helper, t == HELP_AT))(help_out)
        off = sum(jnp.where(t // 4 == i, o, 0) for i, o in enumerate(OFFSETS[:-1]))
        y = wrap(z + off)

        lent = jnp.logical_and(lender, jnp.logical_and(y < LENT, t % 2 == 1))

        @pl.when(jnp.logical_and(need(z, y), jnp.logical_not(lent)))
        def _():
            tiles(y, rows_of(t % 4), UNIT, cols, None)
        return carry

    def sweep_half(h, t, carry):
        for at in SCHEDULE:
            if full + 4 * h <= at < full + 4 * h + 4:
                pl.when(t == at)(lambda: late(at))
        y = wrap(z + OFFSETS[-1])

        @pl.when(need(z, y))
        def _():
            tiles(y, rows_of(t % 4), UNIT, cols // 2, None, h * (cols // 2))
        return carry

    swap_wait()
    lax.fori_loop(0, full, sweep, 0)
    for h in range(2):
        lax.fori_loop(full + 4 * h, full + 4 * h + 4, functools.partial(sweep_half, h), 0)
        home(h, True)
    late(end)

    @pl.when(core == 1)
    def _():
        for p in range(2):
            cross_kv(p).wait_recv()

    crossed = jnp.where(core == 0, z, chips)
    tiles(crossed, rows_of(jnp.where(core == 0, 0, 3)), UNIT, cols, None)
    dq_swap().start()
    pl.when(core == 1)(lambda: cross_sum().start())
    late(end + 1)
    lax.fori_loop(pairs // 2, pairs, functools.partial(diag, cols), 0)
    late(end + 2)

    @pl.when(lender)
    def _():
        give_back().wait_recv()
        r = pl.ds(rows - GROUP, GROUP)
        dq_all[r, :] += lent_dq[...]

    dq_swap().wait_recv()
    for g in range(rows // CHUNK):
        r = pl.ds(g * CHUNK, CHUNK)
        dq_out[r, :] = ((dq_all[r, :] + dq_in[r, :]) * scale).astype(BF16)

    @pl.when(core == 0)
    def _():
        cross_sum().wait_recv()
        part[z] += cross[...]

    for p in range(2):
        @pl.when(up_on(1, z + 1, p))
        def _():
            for h in range(2):
                rs_home(p, h).wait_recv()
            part[z, p] += dn_buf[0, p]

        @pl.when(dn_on(1, z - 1, p))
        def _():
            rs_up(1, p).wait_recv()
            part[z, p] += up_buf[0, p]

    dk_out[...] = (part[z, 0] * scale).T.astype(BF16)
    dv_out[...] = part[z, 1].T.astype(BF16)

    for g in range(halves):
        for i in range(2):
            swap(i, g).wait_send()
    swap_stats().wait_send()

    @pl.when(core == 0)
    def _():
        for p in range(2):
            cross_kv(p).wait_send()

    pl.when(core == 1)(lambda: cross_sum().wait_send())
    for p in range(2):
        for d in range(1, UP[p] + 1):
            pl.when(up_on(d, z + 1, p))(lambda: ag_up(d, p, d - 1).wait_send())
            if d > 1:
                pl.when(up_on(d, z, p))(lambda: rs_dn(d, p).wait_send())
        for h in range(2):
            pl.when(up_on(1, z, p))(lambda: rs_home(p, h).wait_send())
        for e in range(1, DOWN[p] + 1):
            pl.when(dn_on(e, z - 1, p))(lambda: ag_dn(e, p, e - 1).wait_send())
            pl.when(dn_on(e, z, p))(lambda: rs_up(e, p).wait_send())
    dq_swap().wait_send()

    @pl.when(lender)
    def _():
        for i in range(3):
            lend(i).wait_send()

    @pl.when(helper)
    def _():
        for i in range(3):
            pass_on(i).wait_send()
        merge().wait_send()
        give_back().wait_send()


def deliver(dq, dk, dv, dq_out, dk_out, dv_out, sem):
    moves = [pltpu.make_async_copy(s, d, sem.at[i]) for i, (s, d) in enumerate(((dq, dq_out), (dk, dk_out), (dv, dv_out)))]
    for m in moves:
        m.start()
    for m in moves:
        m.wait()


def solution(mesh):
    n = mesh.shape['cp']
    row_spec = P(('dp', 'cp'))

    def local_fn(q_tok, k_tok, v_tok, fwd_out, d_out, lse_row):
        toks, heads, dim = q_tok.shape
        rows = toks * heads
        scale = dim ** -0.5
        flat = lambda x: x.reshape(rows, dim)
        chips = n // 2
        halves = rows // GROUP
        held = 2 * rows + 2 * GROUP
        dma = pltpu.SemaphoreType.DMA
        hbm, vmem = pl.BlockSpec(memory_space=pl.ANY), pl.BlockSpec(memory_space=pltpu.VMEM)
        shapes = (jax.ShapeDtypeStruct((rows, dim), BF16), jax.ShapeDtypeStruct((toks, dim), BF16), jax.ShapeDtypeStruct((toks, dim), BF16))
        hops = dma((FAR, 2))
        grads = pl.pallas_call(
            functools.partial(kernel, n, scale),
            out_shape=tuple(pltpu.VMEM(s.shape, s.dtype) for s in shapes),
            in_specs=[hbm] * 5 + [vmem],
            out_specs=[vmem] * 3,
            scratch_shapes=[
                pltpu.VMEM((held, dim), BF16),
                pltpu.VMEM((held, dim), BF16),
                pltpu.VMEM((rows, dim), BF16),
                pltpu.VMEM((held, 128), F32),
                pltpu.VMEM((held, 128), F32),
                pltpu.VMEM((4, 2, heads, toks), F32),
                pltpu.VMEM((chips + 1, 2, toks, dim), BF16),
                pltpu.VMEM((chips + 1, 2, dim, toks), F32),
                pltpu.VMEM((2, dim, toks), F32),
                pltpu.VMEM((held, dim), F32),
                pltpu.VMEM((GROUP, dim), F32),
                pltpu.VMEM((rows, dim), F32),
                pltpu.VMEM((FAR, 2, dim, toks), F32),
                pltpu.VMEM((FAR, 2, dim, toks), F32),
                dma((5,)), dma((3, halves)), dma((3, halves)),
                hops, hops, hops, hops, hops, hops, hops, hops,
                dma, dma, dma((3,)), dma((3,)), dma((2, 2)), dma((2, 2)),
                dma((3,)), dma((3,)), dma((3,)), dma((3,)), dma((2,)), dma((2,)),
            ],
            compiler_params=pltpu.CompilerParams(collective_id=0, has_side_effects=True, vmem_limit_bytes=60 * 2 ** 20),
        )(flat(q_tok), k_tok, v_tok, flat(fwd_out), flat(d_out), lse_row.T)
        dq, dk, dv = pl.pallas_call(
            deliver,
            out_shape=shapes,
            in_specs=[hbm] * 3,
            out_specs=[hbm] * 3,
            scratch_shapes=[dma((3,))],
        )(*(pltpu.with_memory_space_constraint(g, pltpu.VMEM) for g in grads))
        return dq.reshape(q_tok.shape), dk, dv

    return jax.shard_map(local_fn, mesh=mesh, in_specs=(row_spec,) * 6, out_specs=(row_spec,) * 3, check_vma=False)
```
